128 devices in a mesh: rows: 32 (over z, x, core), grp: 4 (over y).
Axes of the slice: x: 4, y: 4, z: 4, core: 2. Of those that a mesh axis runs over, the one named last changes fastest.
Arguments:
- tiles: bfloat16 [16384, 128, 128], P(('rows', 'grp')), may hold values from -0.3125 to 0.3125
- tile_rows: int32 [16384], P(('rows', 'grp')), may hold values from 0 to 47, as said below
- tile_cols: int32 [16384], P(('rows', 'grp')), may hold values from 0 to 2047, as said below
- tile_count: int32 [128], P(('rows', 'grp')), may hold values from 32 to 128, as said below
- block_perm: int32 [2048], replicated, may hold values from 0 to 2047, as said below
- panel: bfloat16 [2048, 128, 256], P(('rows', 'grp')), may hold values from -6 to 6
Outputs:
- sketch: bfloat16 [6144, 128, 256], P(('rows', 'grp'))
- gram: float32 [2048, 128, 256], P(('rows', 'grp'))
The draws below stay inside these ranges and needn't reach their ends.
Inputs may be any that keep to these rules, and one draw needn't show every extreme that they name: `tile_rows`: each device's live tile rows are non-decreasing; slots past the count hold 47. `tile_cols`: among one device's live tiles, those whose block_perm positions lie with one owner (position // 16) name at most 2 distinct column blocks; every device reaches 2 for some owner. `tile_count`: some device has 128 live tiles. `block_perm`: A permutation of the column blocks.
All inputs are finite; a program needn't handle non-finite values.
Results may differ from the reference program's by a relative error of at most 0.0034.
Values may be sent and summed in bfloat16 or wider, within the bound.
No kernel may reach another device: no remote copies, remote signals or barrier semaphores. Data moves between devices by JAX's collectives and lax.ppermute only.
A program may use at most 128 MiB of HBM per device.

```python
import jax
import jax.numpy as jnp
from jax import lax

BS = 128
K = 256
RB_DEV = 48
TILE_CAP = 128
CB_DEV = 16
PAIR_CAP = 2
NDEV = 128
NCB = 2048


def tile_layout(key):
    base = jax.random.fold_in(key, 7)
    order = jax.random.permutation(jax.random.fold_in(base, 1), NCB).astype(jnp.int32)
    inverse = jnp.argsort(order).astype(jnp.int32)
    first_pick = jax.random.randint(jax.random.fold_in(base, 2), (NDEV, NDEV), 0, CB_DEV).astype(jnp.int32)
    step_pick = jax.random.randint(jax.random.fold_in(base, 8), (NDEV, NDEV), 0, CB_DEV - 1).astype(jnp.int32)
    second_pick = ((first_pick + 1 + step_pick) % CB_DEV).astype(jnp.int32)
    owners = jax.random.randint(jax.random.fold_in(base, 3), (NDEV, TILE_CAP), 0, NDEV).astype(jnp.int32)
    owners = owners.at[:, 1].set(owners[:, 0])
    sides = jax.random.randint(jax.random.fold_in(base, 9), (NDEV, TILE_CAP), 0, 2).astype(jnp.int32)
    sides = sides.at[:, 0].set(0).at[:, 1].set(1)
    source = jnp.arange(NDEV, dtype=jnp.int32)[:, None] + jnp.zeros((NDEV, TILE_CAP), jnp.int32)
    local = jnp.where(sides == 0, first_pick[source, owners], second_pick[source, owners])
    stores = (owners * CB_DEV + local).astype(jnp.int32)
    columns = inverse[stores].astype(jnp.int32)
    raw_rows = jax.random.randint(jax.random.fold_in(base, 4), (NDEV, TILE_CAP), 0, RB_DEV).astype(jnp.int32)
    counts = jax.random.randint(jax.random.fold_in(base, 5), (NDEV,), TILE_CAP // 4, TILE_CAP + 1).astype(jnp.int32)
    fullest = jax.random.randint(jax.random.fold_in(base, 6), (), 0, NDEV)
    counts = jnp.where(jnp.arange(NDEV) == fullest, TILE_CAP, counts).astype(jnp.int32)
    is_live = jnp.arange(TILE_CAP)[None, :] < counts[:, None]
    rows_sorted = jnp.sort(jnp.where(is_live, raw_rows, RB_DEV - 1), axis=1).astype(jnp.int32)
    return (order, columns.reshape(-1), rows_sorted.reshape(-1), counts)


def draw_tile_rows(key, part):
    return tile_layout(key)[2]


def draw_tile_cols(key, part):
    return tile_layout(key)[1]


def draw_tile_count(key, part):
    return tile_layout(key)[3]


def draw_block_perm(key, part):
    return tile_layout(key)[0]


def steps_of(own_key, dims, split, smallest, high):
    level = 1.0
    for axis_at, shards_of in split:
        steps = jax.random.uniform(jax.random.fold_in(jax.random.fold_in(own_key, 6), axis_at), (shards_of,), jnp.float32, smallest / len(split), high / len(split))
        level = level * jnp.repeat(jnp.exp(steps), dims[axis_at] // shards_of).reshape((-1,) + (1,) * (len(dims) - 1 - axis_at))
    return level


def scatter_about(own_key, dims, scale, bound, shards=(), kind=jnp.bfloat16):
    loudness = steps_of(own_key, dims, shards, -0.22, 0.18) if shards else 1.0
    array = jax.random.normal(own_key, dims, jnp.float32) * scale * loudness
    return jnp.minimum(jnp.maximum(array, -bound), bound).astype(kind)


def setup_inputs(seed: int = 0) -> dict:
    splits = jax.random.split(jax.random.key(seed), 7)
    return {
        "tiles": scatter_about(splits[0], (NDEV * TILE_CAP, BS, BS), (BS * TILE_CAP // RB_DEV) ** -0.5, 0.3125, ((0, 128),)),
        "tile_rows": draw_tile_rows(jax.random.fold_in(splits[6], 71), 0),
        "tile_cols": draw_tile_cols(jax.random.fold_in(splits[6], 71), 0),
        "tile_count": draw_tile_count(jax.random.fold_in(splits[6], 71), 0),
        "block_perm": draw_block_perm(jax.random.fold_in(splits[6], 71), 0),
        "panel": scatter_about(splits[5], (NCB, BS, K), 1.0, 6.0, ((0, 128),)),
    }


def block_ranks(stored_at, is_live):
    positions = jnp.arange(NCB, dtype=jnp.int32)
    hits = is_live[:, None] & (stored_at[:, None] == positions[None, :])
    needed = jnp.any(hits, axis=0).reshape(NDEV, CB_DEV)
    ranking = (jnp.cumsum(needed.astype(jnp.int32), axis=1) - 1).astype(jnp.int32)
    local_ids = jnp.arange(CB_DEV, dtype=jnp.int32)
    listed = [jnp.max(jnp.where(needed & (ranking == slot), local_ids[None, :], -1), axis=1) for slot in range(PAIR_CAP)]
    return ranking, jnp.stack(listed, axis=1).astype(jnp.int32)


def reference(tiles, tile_rows, tile_cols, tile_count, block_perm, panel):
    tiles_dev = tiles.reshape(NDEV, TILE_CAP, BS, BS)
    rows_dev = tile_rows.reshape(NDEV, TILE_CAP)
    cols_dev = tile_cols.reshape(NDEV, TILE_CAP)
    slot_ids = jnp.arange(TILE_CAP, dtype=jnp.int32)
    owner_ids = jnp.arange(NDEV, dtype=jnp.int32)

    def one_device(total, inputs):
        block, row_ids, col_ids, count = inputs
        is_live = slot_ids < count
        weight = jnp.where(is_live, 1.0, 0.0).astype(jnp.float32)
        stored_at = block_perm[col_ids].astype(jnp.int32)
        owner_of = (stored_at // CB_DEV).astype(jnp.int32)
        local_block = (stored_at % CB_DEV).astype(jnp.int32)
        ranking, listed = block_ranks(stored_at, is_live)
        slot_of = (owner_of * PAIR_CAP + ranking[owner_of, local_block]).astype(jnp.int32)
        slot_of = jnp.where(is_live, slot_of, 0).astype(jnp.int32)
        block_f = block.astype(jnp.float32)
        fetched = panel[stored_at].astype(jnp.float32)
        product = jnp.einsum("tij,tjk->tik", block_f, fetched)
        sketch_dev = jax.ops.segment_sum(product * weight[:, None, None], row_ids, num_segments=RB_DEV).astype(jnp.bfloat16)
        partial_value = jnp.einsum("tij,tik->tjk", block_f, sketch_dev[row_ids].astype(jnp.float32))
        per_slot = jax.ops.segment_sum(partial_value * weight[:, None, None], slot_of, num_segments=NDEV * PAIR_CAP).astype(jnp.bfloat16)
        flat_list = listed.reshape(-1)
        valid = jnp.where(flat_list >= 0, 1.0, 0.0).astype(jnp.float32)
        target = (jnp.repeat(owner_ids, PAIR_CAP) * CB_DEV + jnp.maximum(flat_list, 0)).astype(jnp.int32)
        total = total.at[target].add(per_slot.astype(jnp.float32) * valid[:, None, None])
        return total, sketch_dev

    zero_gram = jnp.zeros((NCB, BS, K), jnp.float32)
    gram, sketches = lax.scan(one_device, zero_gram, (tiles_dev, rows_dev, cols_dev, tile_count))
    return sketches.reshape(NDEV * RB_DEV, BS, K), gram
```

```python
import functools

import jax
import jax.numpy as jnp
from jax import lax
from jax.experimental import pallas as pl
from jax.experimental.pallas import tpu as pltpu
from jax.sharding import PartitionSpec as P

RB_DEV = 48
AXES = ("rows", "grp")
LANES = 128
CHUNK = 8
GROUP_BITS = 3


def distinct_blocks(stored_at, is_live, total_blocks):
    slots = stored_at.shape[0]
    ids = jnp.arange(slots, dtype=jnp.int32)
    same = (stored_at[:, None] == stored_at[None, :]) & is_live[None, :] & is_live[:, None]
    leader = jnp.min(jnp.where(same, ids[None, :], slots), axis=1)
    is_first = leader == ids
    slot_of = jnp.sum((is_first[None, :] & (ids[None, :] < leader[:, None])).astype(jnp.int32), axis=1)
    slot_of = jnp.where(is_live, slot_of, 0)
    at_slot = is_first[None, :] & (slot_of[None, :] == ids[:, None])
    wanted = jnp.max(jnp.where(at_slot, stored_at[None, :], -1), axis=1)
    wanted = jnp.where(wanted < 0, total_blocks, wanted)
    return wanted, slot_of, is_first.astype(jnp.int32)


def gather_kernel(capacity, want_ref, rows_ref, out_ref, table, stage):
    devices, held = rows_ref.shape[0], 16
    blocks = devices * held

    @pl.when(pl.program_id(0) == 0)
    def _():
        for half in range(2):
            rows = rows_ref[:, half * held : (half + 1) * held, :].astype(jnp.float32)
            table[pl.ds(half, blocks, stride=2), :] = rows.reshape(blocks, LANES)

    for local in range(CHUNK):
        for k in range(capacity):
            src = want_ref[0, 0, local * LANES + k]
            stage[pl.ds(2 * (local * capacity + k), 2), :] = table[pl.ds(src, 2), :]
    span = CHUNK * capacity
    out_ref[:, :LANES] = stage[pl.ds(0, span, stride=2), :].astype(jnp.bfloat16)
    out_ref[:, LANES:] = stage[pl.ds(1, span, stride=2), :].astype(jnp.bfloat16)


def want_blocks(devices):
    return pl.BlockSpec((1, 1, CHUNK * LANES), lambda s: (s, 0, 0), memory_space=pltpu.SMEM)


def gather_rows(want, rows, capacity):
    devices = rows.shape[0]
    blocks = devices * 16
    return pl.pallas_call(
        functools.partial(gather_kernel, capacity),
        grid=(devices // CHUNK,),
        in_specs=[want_blocks(devices), pl.BlockSpec(rows.shape, lambda s: (0, 0, 0))],
        out_specs=pl.BlockSpec((CHUNK * capacity, 2 * LANES), lambda s: (s, 0)),
        out_shape=jax.ShapeDtypeStruct((devices * capacity, 2 * LANES), jnp.bfloat16),
        scratch_shapes=[
            pltpu.VMEM((2 * (blocks + 8), LANES), jnp.float32),
            pltpu.VMEM((2 * CHUNK * capacity, LANES), jnp.float32),
        ],
        compiler_params=pltpu.CompilerParams(vmem_limit_bytes=16 << 20),
        name=f"gather_rows_{capacity}",
    )(want, rows)


def product_kernel(
    capacity, slot_ref, first_ref, row_ref, count_ref, tiles_ref, in_ref, sketch_ref, out_ref,
    in_l, in_r, acc
):
    step = pl.program_id(0)
    span = in_ref.shape[0]
    steps_in = LANES * capacity // span

    @pl.when(step < steps_in)
    def _():
        at = pl.multiple_of(step * span, 8)
        in_l[pl.ds(at, span), :] = in_ref[:, :LANES].astype(jnp.float32)
        in_r[pl.ds(at, span), :] = in_ref[:, LANES:].astype(jnp.float32)

    def forward(first_tile, group):
        products = []
        for t in [first_tile + k for k in range(group)]:
            rows = pl.ds(slot_ref[t], LANES, stride=capacity)
            block = jnp.concatenate(
                [in_l[rows, :].astype(jnp.bfloat16), in_r[rows, :].astype(jnp.bfloat16)], axis=1
            )
            products.append(jnp.dot(tiles_ref[t], block, preferred_element_type=jnp.float32))
        total = acc[...]
        for k, product in enumerate(products):
            t = first_tile + k
            row = row_ref[t]
            fresh = (t == 0) | (row_ref[jnp.maximum(t - 1, 0)] != row)
            total = jnp.where(fresh, product, total + product)
            sketch_ref[row] = total.astype(jnp.bfloat16)
        acc[...] = total

    def backward(first_tile, group):
        parts = []
        for t in [first_tile + k for k in range(group)]:
            parts.append(
                lax.dot_general(
                    tiles_ref[t],
                    sketch_ref[row_ref[t]],
                    (((0,), (0,)), ((), ())),
                    preferred_element_type=jnp.float32,
                )
            )
        for k, part in enumerate(parts):
            t = first_tile + k
            rows = pl.ds(slot_ref[t], LANES, stride=capacity)
            first = first_ref[t] == 1
            in_l[rows, :] = part[:, :LANES] + jnp.where(first, 0.0, in_l[rows, :])
            in_r[rows, :] = part[:, LANES:] + jnp.where(first, 0.0, in_r[rows, :])

    @pl.when(step == steps_in)
    def _():
        count = count_ref[0]
        full = lax.shift_right_logical(count, GROUP_BITS)
        group = 1 << GROUP_BITS
        sketch_ref[...] = jnp.zeros_like(sketch_ref)
        for work in (forward, backward):

            def many(g, carry, work=work):
                work(g * group, group)
                return carry

            def single(t, carry, work=work):
                work(t, 1)
                return carry

            lax.fori_loop(0, full, many, 0)
            lax.fori_loop(full * group, count, single, 0)

    @pl.when(step > steps_in)
    def _():
        at = pl.multiple_of((step - steps_in - 1) * span, 8)
        out_ref[:, :LANES] = in_l[pl.ds(at, span), :].astype(jnp.bfloat16)
        out_ref[:, LANES:] = in_r[pl.ds(at, span), :].astype(jnp.bfloat16)


def tile_products(slot_of, is_first, tile_rows, tile_count, tiles, fetched, capacity):
    steps = 8
    span = LANES // steps * capacity
    scalars = [pl.BlockSpec(memory_space=pltpu.SMEM)] * 4
    f32_rows = pltpu.VMEM((LANES * capacity, LANES), jnp.float32)
    return pl.pallas_call(
        functools.partial(product_kernel, capacity),
        grid=(2 * steps + 1,),
        in_specs=scalars
        + [
            pl.BlockSpec(tiles.shape, lambda s: (0, 0, 0), pipeline_mode=pl.Buffered(1)),
            pl.BlockSpec((span, 2 * LANES), lambda s: (jnp.minimum(s, steps - 1), 0)),
        ],
        out_specs=[
            pl.BlockSpec((RB_DEV, LANES, 2 * LANES), lambda s: (0, 0, 0), pipeline_mode=pl.Buffered(1)),
            pl.BlockSpec((span, 2 * LANES), lambda s: (jnp.maximum(s - steps - 1, 0), 0)),
        ],
        out_shape=[
            jax.ShapeDtypeStruct((RB_DEV, LANES, 2 * LANES), jnp.bfloat16),
            jax.ShapeDtypeStruct((LANES * capacity, 2 * LANES), jnp.bfloat16),
        ],
        scratch_shapes=[
            f32_rows,
            f32_rows,
            pltpu.VMEM((LANES, 2 * LANES), jnp.float32),
        ],
        compiler_params=pltpu.CompilerParams(vmem_limit_bytes=36 << 20),
        name=f"tile_products_{capacity}",
    )(slot_of, is_first, tile_rows, tile_count, tiles, fetched)


def sum_kernel(capacity, want_ref, in_ref, out_ref, total, stage):
    step = pl.program_id(0)
    span = CHUNK * capacity

    @pl.when(step == 0)
    def _():
        total[...] = jnp.zeros_like(total)

    stage[pl.ds(0, span, stride=2), :] = in_ref[:, :LANES].astype(jnp.float32)
    stage[pl.ds(1, span, stride=2), :] = in_ref[:, LANES:].astype(jnp.float32)
    for local in range(CHUNK):

        def load(g, local=local):
            loaded = []
            for k in range(g * 8, g * 8 + 8):
                w = want_ref[0, 0, local * LANES + k]
                loaded.append((w, total[pl.ds(w, 2), :], stage[pl.ds(2 * (local * capacity + k), 2), :]))
            return loaded

        ahead = load(0)
        for g in range(capacity // 8):
            now, ahead = ahead, load(g + 1) if g + 1 < capacity // 8 else None
            for w, old, row in now:
                total[pl.ds(w, 2), :] = old + row

    @pl.when(step == pl.num_programs(0) - 1)
    def _():
        blocks = out_ref.shape[0]
        out_ref[:, :LANES] = total[pl.ds(0, blocks, stride=2), :].astype(jnp.bfloat16)
        out_ref[:, LANES:] = total[pl.ds(1, blocks, stride=2), :].astype(jnp.bfloat16)


def sum_rows(want, inbound, capacity, devices):
    blocks = devices * 16
    return pl.pallas_call(
        functools.partial(sum_kernel, capacity),
        grid=(devices // CHUNK,),
        in_specs=[want_blocks(devices), pl.BlockSpec((CHUNK * capacity, 2 * LANES), lambda s: (s, 0))],
        out_specs=pl.BlockSpec((blocks, 2 * LANES), lambda s: (0, 0)),
        out_shape=jax.ShapeDtypeStruct((blocks, 2 * LANES), jnp.bfloat16),
        scratch_shapes=[
            pltpu.VMEM((2 * (blocks + 8), LANES), jnp.float32),
            pltpu.VMEM((2 * CHUNK * capacity, LANES), jnp.float32),
        ],
        compiler_params=pltpu.CompilerParams(vmem_limit_bytes=16 << 20),
        name=f"sum_rows_{capacity}",
    )(want, inbound)


def exchange(x):
    return lax.all_to_all(x, AXES, split_axis=0, concat_axis=0, tiled=True)


def per_device(tiles, tile_rows, tile_cols, tile_count, block_perm, panel):
    devices = lax.axis_size(AXES)
    held = panel.shape[0]
    blocks = devices * held
    slot_ids = jnp.arange(tiles.shape[0], dtype=jnp.int32)
    is_live = slot_ids < tile_count[0]
    stored_at = block_perm[tile_cols]
    wanted, slot_of, is_first = distinct_blocks(stored_at, is_live, blocks)

    digits = jnp.stack([wanted // held, wanted % held]).astype(jnp.bfloat16)
    stripes = panel.reshape(held, devices, 2, LANES).transpose(1, 2, 0, 3).reshape(devices, 2 * held, LANES)
    stripes = jnp.concatenate([stripes, jnp.broadcast_to(digits[None], (devices, 2, LANES))], axis=1)
    striped = exchange(stripes)
    lists = striped[:, 2 * held :, :].astype(jnp.int32)
    want = (lists[:, 0] * held + lists[:, 1])
    counts = jnp.sum((want < blocks).astype(jnp.int32), axis=1)
    want = (2 * want).reshape(devices // CHUNK, 1, CHUNK * LANES)

    def with_capacity(capacity):
        def run():
            outgoing = gather_rows(want, striped, capacity)
            fetched = exchange(outgoing.reshape(devices, capacity, 2 * LANES))
            sketch, outbound = tile_products(
                slot_of, is_first, tile_rows, tile_count, tiles,
                fetched.reshape(devices * capacity, 2 * LANES), capacity,
            )
            inbound = exchange(outbound.reshape(devices, capacity, 2 * LANES))
            summed = sum_rows(want, inbound.reshape(devices * capacity, 2 * LANES), capacity, devices)
            return sketch, summed

        return run

    sketch, summed = lax.cond(jnp.max(counts) <= 112, with_capacity(112), with_capacity(128))
    gram = exchange(summed.reshape(devices, held, 2 * LANES))
    return sketch, gram.transpose(1, 0, 2).astype(jnp.float32)


def solution(mesh):
    split = P(AXES, None, None)
    line = P(AXES)
    return jax.shard_map(
        per_device,
        mesh=mesh,
        in_specs=(split, line, line, line, P(), split),
        out_specs=(split, split),
        check_vma=False,
    )
```

```python
import functools

import jax
import jax.numpy as jnp
from jax import lax
from jax.experimental import pallas as pl
from jax.experimental.pallas import tpu as pltpu
from jax.sharding import PartitionSpec as P

RB_DEV = 48
AXES = ("rows", "grp")
LANES = 128
CHUNK = 8
GROUP_BITS = 3
SUM_GROUP = 8
GRANT = 12
PRODUCT_GRANT = 24
CAPACITIES = (104, 112, 128)


def distinct_blocks(stored_at, is_live, total_blocks):
    slots = stored_at.shape[0]
    ids = jnp.arange(slots, dtype=jnp.int32)
    same = (stored_at[:, None] == stored_at[None, :]) & is_live[None, :] & is_live[:, None]
    leader = jnp.min(jnp.where(same, ids[None, :], slots), axis=1)
    is_first = leader == ids
    slot_of = jnp.sum((is_first[None, :] & (ids[None, :] < leader[:, None])).astype(jnp.int32), axis=1)
    slot_of = jnp.where(is_live, slot_of, 0)
    at_slot = is_first[None, :] & (slot_of[None, :] == ids[:, None])
    wanted = jnp.max(jnp.where(at_slot, stored_at[None, :], -1), axis=1)
    wanted = jnp.where(wanted < 0, total_blocks, wanted)
    return wanted, slot_of, is_first.astype(jnp.int32)


def chunk_lists(want_ref, buffers, semaphores, work):
    chunks = want_ref.shape[0]

    def copy(chunk, side):
        return pltpu.make_async_copy(want_ref.at[chunk], buffers[side], semaphores.at[side])

    for side in range(2):
        copy(side, side).start()

    def pair(p, carry):
        for side in range(2):
            chunk = 2 * p + side
            copy(chunk, side).wait()
            work(chunk, buffers[side])

            @pl.when(chunk + 2 < chunks)
            def _(chunk=chunk, side=side):
                copy(chunk + 2, side).start()

        return carry

    lax.fori_loop(0, chunks // 2, pair, 0)


def spans(capacity):
    marks = [0] + [m for m in (56, 80) if m < capacity] + [capacity]
    return list(zip(marks[:-1], marks[1:]))


def when_listed(listed, local, start, absent, work):
    if start == 0:
        work()
    else:
        pl.when(listed[local, start] < absent)(work)


def gather_kernel(capacity, want_ref, rows_ref, out_ref, table, stage, list_a, list_b, semaphores):
    devices, held = rows_ref.shape[0], 16
    blocks = devices * held
    span = CHUNK * capacity
    for half in range(2):
        rows = rows_ref[:, half * held : (half + 1) * held, :].astype(jnp.float32)
        table[pl.ds(half, blocks, stride=2), :] = rows.reshape(blocks, LANES)

    def work(chunk, listed):
        for local in range(CHUNK):
            for start, stop in spans(capacity):

                def rows(local=local, start=start, stop=stop):
                    for k in range(start, stop):
                        src = listed[local, k]
                        stage[pl.ds(2 * (local * capacity + k), 2), :] = table[pl.ds(src, 2), :]

                when_listed(listed, local, start, 2 * blocks, rows)
        at = pl.multiple_of(chunk * span, 16)
        out_ref[pl.ds(at, span), :LANES] = stage[pl.ds(0, span, stride=2), :].astype(jnp.bfloat16)
        out_ref[pl.ds(at, span), LANES:] = stage[pl.ds(1, span, stride=2), :].astype(jnp.bfloat16)

    chunk_lists(want_ref, (list_a, list_b), semaphores, work)


def row_scratch(blocks, capacity, tables=1):
    lists = pltpu.SMEM((CHUNK, LANES), jnp.int32)
    table = pltpu.VMEM((2 * (blocks + 8), LANES), jnp.float32)
    return [table] * tables + [
        pltpu.VMEM((2 * CHUNK * capacity, LANES), jnp.float32),
        lists,
        lists,
        pltpu.SemaphoreType.DMA((2,)),
    ]


def gather_rows(want, rows, capacity):
    devices = rows.shape[0]
    return pl.pallas_call(
        functools.partial(gather_kernel, capacity),
        in_specs=[pl.BlockSpec(memory_space=pl.ANY), pl.BlockSpec(memory_space=pltpu.VMEM)],
        out_specs=pl.BlockSpec(memory_space=pltpu.VMEM),
        out_shape=jax.ShapeDtypeStruct((devices * capacity, 2 * LANES), jnp.bfloat16),
        scratch_shapes=row_scratch(devices * 16, capacity),
        compiler_params=pltpu.CompilerParams(vmem_limit_bytes=GRANT << 20),
        name=f"gather_rows_{capacity}",
    )(want, rows)


def product_kernel(
    capacity, slot_ref, first_ref, row_ref, count_ref, tiles_ref, in_ref, sketch_ref, out_ref,
    in_l, in_r, acc, sketch, sent
):
    stride = capacity + 1
    count = count_ref[0]
    full = lax.shift_right_logical(count, GROUP_BITS)
    group = 1 << GROUP_BITS
    halves = ((in_l, pl.ds(0, LANES)), (in_r, pl.ds(LANES, LANES)))

    def spread(c, carry):
        for k in range(CHUNK):
            source = pl.ds(pl.multiple_of((c * CHUNK + k) * capacity, 8), capacity)
            for half, lanes in halves:
                half[pl.ds((c * CHUNK + k) * stride, capacity), :] = in_ref[source, lanes].astype(jnp.float32)
        return carry

    def pack(c, carry):
        for k in range(CHUNK):
            target = pl.ds(pl.multiple_of((c * CHUNK + k) * capacity, 8), capacity)
            for half, lanes in halves:
                out_ref[target, lanes] = half[pl.ds((c * CHUNK + k) * stride, capacity), :].astype(jnp.bfloat16)
        return carry

    def forward(first_tile, group):
        products = []
        for t in [first_tile + k for k in range(group)]:
            rows = pl.ds(slot_ref[t], LANES, stride=stride)
            block = jnp.concatenate([half[rows, :].astype(jnp.bfloat16) for half, _ in halves], axis=1)
            products.append(jnp.dot(tiles_ref[t], block, preferred_element_type=jnp.float32))
        total = acc[...]
        for k, product in enumerate(products):
            t = first_tile + k
            row = row_ref[t]
            fresh = (t == 0) | (row_ref[jnp.maximum(t - 1, 0)] != row)
            total = jnp.where(fresh, product, total + product)
            sketch[row] = total.astype(jnp.bfloat16)
        acc[...] = total

    def backward(first_tile, group):
        parts = []
        for t in [first_tile + k for k in range(group)]:
            parts.append(
                lax.dot_general(
                    tiles_ref[t],
                    sketch[row_ref[t]],
                    (((0,), (0,)), ((), ())),
                    preferred_element_type=jnp.float32,
                )
            )
        for k, part in enumerate(parts):
            t = first_tile + k
            rows = pl.ds(slot_ref[t], LANES, stride=stride)
            first = first_ref[t] == 1
            for (half, _), piece in zip(halves, (part[:, :LANES], part[:, LANES:])):
                half[rows, :] = piece + jnp.where(first, 0.0, half[rows, :])

    def over_tiles(work):
        def many(g, carry):
            work(g * group, group)
            return carry

        def single(t, carry):
            work(t, 1)
            return carry

        lax.fori_loop(0, full, many, 0)
        lax.fori_loop(full * group, count, single, 0)

    sketch[...] = jnp.zeros_like(sketch)
    lax.fori_loop(0, LANES // CHUNK, spread, 0)
    over_tiles(forward)
    send = pltpu.make_async_copy(sketch, sketch_ref, sent)
    send.start()
    over_tiles(backward)
    lax.fori_loop(0, LANES // CHUNK, pack, 0)
    send.wait()


def tile_products(slot_of, is_first, tile_rows, tile_count, tiles, fetched, capacity):
    f32_rows = pltpu.VMEM((LANES * (capacity + 1), LANES), jnp.float32)
    sketch = (RB_DEV, LANES, 2 * LANES)
    return pl.pallas_call(
        functools.partial(product_kernel, capacity),
        in_specs=[pl.BlockSpec(memory_space=pltpu.SMEM)] * 4
        + [pl.BlockSpec(memory_space=pltpu.VMEM)] * 2,
        out_specs=[pl.BlockSpec(memory_space=pl.ANY), pl.BlockSpec(memory_space=pltpu.VMEM)],
        out_shape=[
            jax.ShapeDtypeStruct(sketch, jnp.bfloat16),
            jax.ShapeDtypeStruct((LANES * capacity, 2 * LANES), jnp.bfloat16),
        ],
        scratch_shapes=[
            f32_rows,
            f32_rows,
            pltpu.VMEM((LANES, 2 * LANES), jnp.float32),
            pltpu.VMEM(sketch, jnp.bfloat16),
            pltpu.SemaphoreType.DMA,
        ],
        compiler_params=pltpu.CompilerParams(vmem_limit_bytes=PRODUCT_GRANT << 20),
        name=f"tile_products_{capacity}",
    )(slot_of, is_first, tile_rows, tile_count, tiles, fetched)


def sum_kernel(capacity, want_ref, in_ref, out_ref, even, odd, stage, list_a, list_b, semaphores):
    span = CHUNK * capacity
    blocks = out_ref.shape[0]
    even[...] = jnp.zeros_like(even)
    odd[...] = jnp.zeros_like(odd)

    def work(chunk, listed):
        at = pl.multiple_of(chunk * span, 16)
        stage[pl.ds(0, span, stride=2), :] = in_ref[pl.ds(at, span), :LANES].astype(jnp.float32)
        stage[pl.ds(1, span, stride=2), :] = in_ref[pl.ds(at, span), LANES:].astype(jnp.float32)
        for local in range(0, CHUNK, 2):
            totals = (even, odd)

            def load(side, g, stop, local=local):
                loaded = []
                for k in range(g, min(g + SUM_GROUP, stop)):
                    w = listed[local + side, k]
                    row = stage[pl.ds(2 * ((local + side) * capacity + k), 2), :]
                    loaded.append((w, totals[side][pl.ds(w, 2), :], row))
                return loaded

            def store(side, loaded):
                for w, old, row in loaded:
                    totals[side][pl.ds(w, 2), :] = old + row

            for start, stop in spans(capacity):

                def rows(start=start, stop=stop, load=load):
                    last = load(0, start, stop)
                    turns = [(side, g) for g in range(start, stop, SUM_GROUP) for side in range(2)]
                    for here, ahead in zip(turns, turns[1:] + [None]):
                        following = load(*ahead, stop) if ahead else None
                        store(here[0], last)
                        last = following

                if start == 0:
                    rows()
                else:
                    longest = jnp.minimum(listed[local, start], listed[local + 1, start])
                    pl.when(longest < 2 * blocks)(rows)

    chunk_lists(want_ref, (list_a, list_b), semaphores, work)
    for half in range(2):
        rows = pl.ds(half, blocks, stride=2)
        out_ref[:, half * LANES : (half + 1) * LANES] = (even[rows, :] + odd[rows, :]).astype(jnp.bfloat16)


def sum_rows(want, inbound, capacity, devices):
    blocks = devices * 16
    return pl.pallas_call(
        functools.partial(sum_kernel, capacity),
        in_specs=[pl.BlockSpec(memory_space=pl.ANY), pl.BlockSpec(memory_space=pltpu.VMEM)],
        out_specs=pl.BlockSpec(memory_space=pltpu.VMEM),
        out_shape=jax.ShapeDtypeStruct((blocks, 2 * LANES), jnp.bfloat16),
        scratch_shapes=row_scratch(blocks, capacity, 2),
        compiler_params=pltpu.CompilerParams(vmem_limit_bytes=GRANT << 20),
        name=f"sum_rows_{capacity}",
    )(want, inbound)


def exchange(x):
    return lax.all_to_all(x, AXES, split_axis=0, concat_axis=0, tiled=True)


def per_device(tiles, tile_rows, tile_cols, tile_count, block_perm, panel):
    devices = lax.axis_size(AXES)
    held = panel.shape[0]
    blocks = devices * held
    slot_ids = jnp.arange(tiles.shape[0], dtype=jnp.int32)
    is_live = slot_ids < tile_count[0]
    stored_at = block_perm[tile_cols]
    wanted, slot_of, is_first = distinct_blocks(stored_at, is_live, blocks)

    digits = jnp.stack([wanted // held, wanted % held]).astype(jnp.bfloat16)
    stripes = panel.reshape(held, devices, 2, LANES).transpose(1, 2, 0, 3).reshape(devices, 2 * held, LANES)
    stripes = jnp.concatenate([stripes, jnp.broadcast_to(digits[None], (devices, 2, LANES))], axis=1)
    striped = exchange(stripes)
    lists = striped[:, 2 * held :, :].astype(jnp.int32)
    want = (lists[:, 0] * held + lists[:, 1])
    counts = jnp.sum((want < blocks).astype(jnp.int32), axis=1)
    want = (2 * want).reshape(devices // CHUNK, CHUNK, LANES)

    def with_capacity(capacity):
        def run():
            outgoing = gather_rows(want, striped, capacity)
            fetched = exchange(outgoing.reshape(devices, capacity, 2 * LANES))
            sketch, outbound = tile_products(
                slot_of, is_first, tile_rows, tile_count, tiles,
                fetched.reshape(devices * capacity, 2 * LANES), capacity,
            )
            inbound = exchange(outbound.reshape(devices, capacity, 2 * LANES))
            summed = sum_rows(want, inbound.reshape(devices * capacity, 2 * LANES), capacity, devices)
            return sketch, summed

        return run

    most = jnp.max(counts)
    choice = sum((most > c).astype(jnp.int32) for c in CAPACITIES[:-1])
    sketch, summed = lax.switch(choice, [with_capacity(c) for c in CAPACITIES])
    gram = exchange(summed.reshape(devices, held, 2 * LANES))
    return sketch, gram.transpose(1, 0, 2).astype(jnp.float32)


def solution(mesh):
    split = P(AXES, None, None)
    line = P(AXES)
    return jax.shard_map(
        per_device,
        mesh=mesh,
        in_specs=(split, line, line, line, P(), split),
        out_specs=(split, split),
        check_vma=False,
    )
```

```python
import functools

import jax
import jax.numpy as jnp
from jax import lax
from jax.experimental import pallas as pl
from jax.experimental.pallas import tpu as pltpu
from jax.sharding import PartitionSpec as P

RB_DEV = 48
AXES = ("rows", "grp")
LANES = 128
CHUNK = 8
GROUP_BITS = 3
SUM_GROUP = 8
GRANT = 12
PRODUCT_GRANT = 28
CAPACITIES = (104, 108, 112, 128)


def distinct_blocks(stored_at, is_live, total_blocks):
    slots = stored_at.shape[0]
    ids = jnp.arange(slots, dtype=jnp.int32)
    same = (stored_at[:, None] == stored_at[None, :]) & is_live[None, :] & is_live[:, None]
    leader = jnp.min(jnp.where(same, ids[None, :], slots), axis=1)
    is_first = leader == ids
    slot_of = jnp.sum((is_first[None, :] & (ids[None, :] < leader[:, None])).astype(jnp.int32), axis=1)
    slot_of = jnp.where(is_live, slot_of, 0)
    at_slot = is_first[None, :] & (slot_of[None, :] == ids[:, None])
    wanted = jnp.max(jnp.where(at_slot, stored_at[None, :], -1), axis=1)
    wanted = jnp.where(wanted < 0, total_blocks, wanted)
    return wanted, slot_of, is_first.astype(jnp.int32)


def chunk_lists(want_ref, buffers, semaphores, work):
    chunks = want_ref.shape[0] // CHUNK

    def copy(chunk, side):
        source = want_ref.at[pl.ds(pl.multiple_of(chunk * CHUNK, CHUNK), CHUNK)]
        return pltpu.make_async_copy(source, buffers[side], semaphores.at[side])

    for side in range(2):
        copy(side, side).start()

    def pair(p, carry):
        for side in range(2):
            chunk = 2 * p + side
            copy(chunk, side).wait()
            work(chunk, buffers[side])

            @pl.when(chunk + 2 < chunks)
            def _(chunk=chunk, side=side):
                copy(chunk + 2, side).start()

        return carry

    lax.fori_loop(0, chunks // 2, pair, 0)


def spans(capacity):
    marks = [0] + [m for m in (56, 80) if m < capacity] + [capacity]
    return list(zip(marks[:-1], marks[1:]))


def when_listed(listed, local, start, absent, work):
    if start == 0:
        work()
    else:
        pl.when(listed[local, start] < absent)(work)


def gather_kernel(capacity, rows_ref, out_ref, want_ref, table, digits, stage, list_a, list_b, semaphores):
    devices, held = rows_ref.shape[0], 16
    blocks = devices * held
    span = 2 * CHUNK * capacity
    digits[...] = rows_ref[:, 2 * held :, :].astype(jnp.float32).reshape(devices * 8, LANES)
    high = digits[pl.ds(0, devices, stride=8), :]
    low = digits[pl.ds(1, devices, stride=8), :]
    want_ref[...] = (2 * (high * held + low)).astype(jnp.int32)
    for half in range(2):
        rows = rows_ref[:, half * held : (half + 1) * held, :].astype(jnp.float32)
        table[pl.ds(half, blocks, stride=2), :] = rows.reshape(blocks, LANES)

    def work(chunk, listed):
        for local in range(CHUNK):
            for start, stop in spans(capacity):

                def rows(local=local, start=start, stop=stop):
                    for k in range(start, stop):
                        src = listed[local, k]
                        stage[pl.ds(2 * (local * capacity + k), 2), :] = table[pl.ds(src, 2), :]

                when_listed(listed, local, start, 2 * blocks, rows)
        out_ref[pl.ds(pl.multiple_of(chunk * span, 16), span), :] = stage[...].astype(jnp.bfloat16)

    chunk_lists(want_ref, (list_a, list_b), semaphores, work)


def row_table(blocks):
    return pltpu.VMEM((2 * (blocks + 8), LANES), jnp.float32)


def list_scratch(capacity):
    lists = pltpu.SMEM((CHUNK, LANES), jnp.int32)
    stage = pltpu.VMEM((2 * CHUNK * capacity, LANES), jnp.float32)
    return [stage, lists, lists, pltpu.SemaphoreType.DMA((2,))]


def gather_rows(rows, capacity):
    devices = rows.shape[0]
    return pl.pallas_call(
        functools.partial(gather_kernel, capacity),
        in_specs=[pl.BlockSpec(memory_space=pltpu.VMEM)],
        out_specs=[pl.BlockSpec(memory_space=pltpu.VMEM)] * 2,
        out_shape=[
            jax.ShapeDtypeStruct((devices * 2 * capacity, LANES), jnp.bfloat16),
            jax.ShapeDtypeStruct((devices, LANES), jnp.int32),
        ],
        scratch_shapes=[row_table(devices * 16), pltpu.VMEM((devices * 8, LANES), jnp.float32)]
        + list_scratch(capacity),
        compiler_params=pltpu.CompilerParams(vmem_limit_bytes=GRANT << 20),
        name=f"gather_rows_{capacity}",
    )(rows)


def product_kernel(
    capacity, slot_ref, first_ref, row_ref, count_ref, tiles_ref, in_ref, sketch_ref, out_ref,
    spread_rows, acc, sketch, sent
):
    width = 2 * capacity
    stride = width + 1
    count = count_ref[0]
    full = lax.shift_right_logical(count, GROUP_BITS)
    group = 1 << GROUP_BITS

    def spread(c, carry):
        for k in range(CHUNK):
            j = c * CHUNK + k
            source = pl.ds(pl.multiple_of(j * width, 8), width)
            spread_rows[pl.ds(j * stride, width), :] = in_ref[source, :].astype(jnp.float32)
        return carry

    def pack(c, carry):
        for k in range(CHUNK):
            j = c * CHUNK + k
            target = pl.ds(pl.multiple_of(j * width, 8), width)
            out_ref[target, :] = spread_rows[pl.ds(j * stride, width), :].astype(jnp.bfloat16)
        return carry

    def block_rows(t):
        return [pl.ds(2 * slot_ref[t] + half, LANES, stride=stride) for half in range(2)]

    def forward(first_tile, group):
        products = []
        for t in [first_tile + k for k in range(group)]:
            block = [spread_rows[rows, :].astype(jnp.bfloat16) for rows in block_rows(t)]
            block = jnp.concatenate(block, axis=1)
            products.append(jnp.dot(tiles_ref[t], block, preferred_element_type=jnp.float32))
        total = acc[...]
        for k, product in enumerate(products):
            t = first_tile + k
            row = row_ref[t]
            fresh = (t == 0) | (row_ref[jnp.maximum(t - 1, 0)] != row)
            total = jnp.where(fresh, product, total + product)
            sketch[row] = total.astype(jnp.bfloat16)
        acc[...] = total

    def backward(first_tile, group):
        parts = []
        for t in [first_tile + k for k in range(group)]:
            parts.append(
                lax.dot_general(
                    tiles_ref[t],
                    sketch[row_ref[t]],
                    (((0,), (0,)), ((), ())),
                    preferred_element_type=jnp.float32,
                )
            )
        for k, part in enumerate(parts):
            t = first_tile + k
            first = first_ref[t] == 1
            for rows, piece in zip(block_rows(t), (part[:, :LANES], part[:, LANES:])):
                spread_rows[rows, :] = piece + jnp.where(first, 0.0, spread_rows[rows, :])

    def over_tiles(work):
        def many(g, carry):
            work(g * group, group)
            return carry

        def single(t, carry):
            work(t, 1)
            return carry

        lax.fori_loop(0, full, many, 0)
        lax.fori_loop(full * group, count, single, 0)

    sketch[...] = jnp.zeros_like(sketch)
    lax.fori_loop(0, LANES // CHUNK, spread, 0)
    over_tiles(forward)
    send = pltpu.make_async_copy(sketch, sketch_ref, sent)
    send.start()
    over_tiles(backward)
    lax.fori_loop(0, LANES // CHUNK, pack, 0)
    send.wait()


def tile_products(slot_of, is_first, tile_rows, tile_count, tiles, fetched, capacity):
    sketch = (RB_DEV, LANES, 2 * LANES)
    return pl.pallas_call(
        functools.partial(product_kernel, capacity),
        in_specs=[pl.BlockSpec(memory_space=pltpu.SMEM)] * 4
        + [pl.BlockSpec(memory_space=pltpu.VMEM)] * 2,
        out_specs=[pl.BlockSpec(memory_space=pl.ANY), pl.BlockSpec(memory_space=pltpu.VMEM)],
        out_shape=[
            jax.ShapeDtypeStruct(sketch, jnp.bfloat16),
            jax.ShapeDtypeStruct(fetched.shape, jnp.bfloat16),
        ],
        scratch_shapes=[
            pltpu.VMEM((LANES * (2 * capacity + 1) + 8, LANES), jnp.float32),
            pltpu.VMEM((LANES, 2 * LANES), jnp.float32),
            pltpu.VMEM(sketch, jnp.bfloat16),
            pltpu.SemaphoreType.DMA,
        ],
        compiler_params=pltpu.CompilerParams(vmem_limit_bytes=PRODUCT_GRANT << 20),
        name=f"tile_products_{capacity}",
    )(slot_of, is_first, tile_rows, tile_count, tiles, fetched)


def sum_kernel(capacity, want_ref, in_ref, out_ref, even, odd, stage, list_a, list_b, semaphores):
    span = 2 * CHUNK * capacity
    blocks = out_ref.shape[0]
    even[...] = jnp.zeros_like(even)
    odd[...] = jnp.zeros_like(odd)
    totals = (even, odd)

    def work(chunk, listed):
        stage[...] = in_ref[pl.ds(pl.multiple_of(chunk * span, 16), span), :].astype(jnp.float32)
        for local in range(0, CHUNK, 2):

            def load(side, g, stop, local=local):
                loaded = []
                for k in range(g, min(g + SUM_GROUP, stop)):
                    w = listed[local + side, k]
                    row = stage[pl.ds(2 * ((local + side) * capacity + k), 2), :]
                    loaded.append((w, totals[side][pl.ds(w, 2), :], row))
                return loaded

            def store(side, loaded):
                for w, old, row in loaded:
                    totals[side][pl.ds(w, 2), :] = old + row

            for start, stop in spans(capacity):

                def rows(start=start, stop=stop, load=load):
                    last = load(0, start, stop)
                    turns = [(side, g) for g in range(start, stop, SUM_GROUP) for side in range(2)]
                    for here, ahead in zip(turns, turns[1:] + [None]):
                        following = load(*ahead, stop) if ahead else None
                        store(here[0], last)
                        last = following

                if start == 0:
                    rows()
                else:
                    longest = jnp.minimum(listed[local, start], listed[local + 1, start])
                    pl.when(longest < 2 * blocks)(rows)

    chunk_lists(want_ref, (list_a, list_b), semaphores, work)
    for half in range(2):
        rows = pl.ds(half, blocks, stride=2)
        out_ref[:, half * LANES : (half + 1) * LANES] = (even[rows, :] + odd[rows, :]).astype(jnp.bfloat16)


def sum_rows(want, inbound, capacity):
    blocks = want.shape[0] * 16
    return pl.pallas_call(
        functools.partial(sum_kernel, capacity),
        in_specs=[pl.BlockSpec(memory_space=pltpu.VMEM)] * 2,
        out_specs=pl.BlockSpec(memory_space=pltpu.VMEM),
        out_shape=jax.ShapeDtypeStruct((blocks, 2 * LANES), jnp.bfloat16),
        scratch_shapes=[row_table(blocks)] * 2 + list_scratch(capacity),
        compiler_params=pltpu.CompilerParams(vmem_limit_bytes=GRANT << 20),
        name=f"sum_rows_{capacity}",
    )(want, inbound)


def exchange(x):
    return lax.all_to_all(x, AXES, split_axis=0, concat_axis=0, tiled=True)


def per_device(tiles, tile_rows, tile_cols, tile_count, block_perm, panel):
    devices = lax.axis_size(AXES)
    held = panel.shape[0]
    blocks = devices * held
    slot_ids = jnp.arange(tiles.shape[0], dtype=jnp.int32)
    is_live = slot_ids < tile_count[0]
    stored_at = block_perm[tile_cols]
    wanted, slot_of, is_first = distinct_blocks(stored_at, is_live, blocks)

    listed = jnp.sum(is_first)
    notes = [wanted // held, wanted % held, jnp.full_like(wanted, listed)]
    notes = jnp.stack(notes + [jnp.zeros_like(wanted)] * 5).astype(jnp.bfloat16)
    stripes = panel.reshape(held, devices, 2, LANES).transpose(1, 2, 0, 3).reshape(devices, 2 * held, LANES)
    stripes = jnp.concatenate([stripes, jnp.broadcast_to(notes[None], (devices, 8, LANES))], axis=1)
    striped = exchange(stripes)
    most = jnp.max(striped[:, 2 * held + 2, 0]).astype(jnp.int32)

    def with_capacity(capacity):
        def run():
            outgoing, want = gather_rows(striped, capacity)
            fetched = exchange(outgoing.reshape(devices, 2 * capacity, LANES))
            sketch, outbound = tile_products(
                slot_of, is_first, tile_rows, tile_count, tiles, fetched.reshape(outgoing.shape), capacity
            )
            inbound = exchange(outbound.reshape(devices, 2 * capacity, LANES))
            return sketch, sum_rows(want, inbound.reshape(outgoing.shape), capacity)

        return run

    choice = sum((most > c).astype(jnp.int32) for c in CAPACITIES[:-1])
    sketch, summed = lax.switch(choice, [with_capacity(c) for c in CAPACITIES])
    gram = exchange(summed.reshape(devices, held, 2 * LANES))
    return sketch, gram.transpose(1, 0, 2).astype(jnp.float32)


def solution(mesh):
    split = P(AXES, None, None)
    line = P(AXES)
    return jax.shard_map(
        per_device,
        mesh=mesh,
        in_specs=(split, line, line, line, P(), split),
        out_specs=(split, split),
        check_vma=False,
    )
```

```python
import functools

import jax
import jax.numpy as jnp
from jax import lax
from jax.experimental import pallas as pl
from jax.experimental.pallas import tpu as pltpu
from jax.sharding import PartitionSpec as P

RB_DEV = 48
AXES = ("rows", "grp")
LANES = 128
CHUNK = 8
GROUP_BITS = 3
SUM_GROUP = 8
GRANT = 12
PRODUCT_GRANT = 28
CAPACITIES = (104, 108, 112, 128)


def distinct_blocks(stored_at, is_live, total_blocks):
    slots = stored_at.shape[0]
    ids = jnp.arange(slots, dtype=jnp.int32)
    same = (stored_at[:, None] == stored_at[None, :]) & is_live[None, :] & is_live[:, None]
    leader = jnp.min(jnp.where(same, ids[None, :], slots), axis=1)
    is_first = leader == ids
    slot_of = jnp.sum((is_first[None, :] & (ids[None, :] < leader[:, None])).astype(jnp.int32), axis=1)
    slot_of = jnp.where(is_live, slot_of, 0)
    at_slot = is_first[None, :] & (slot_of[None, :] == ids[:, None])
    wanted = jnp.max(jnp.where(at_slot, stored_at[None, :], -1), axis=1)
    wanted = jnp.where(wanted < 0, total_blocks, wanted)
    return wanted, slot_of, is_first.astype(jnp.int32)


def chunk_lists(want_ref, buffers, semaphores, work):
    chunks = want_ref.shape[0] // CHUNK

    def copy(chunk, side):
        source = want_ref.at[pl.ds(pl.multiple_of(chunk * CHUNK, CHUNK), CHUNK)]
        return pltpu.make_async_copy(source, buffers[side], semaphores.at[side])

    for side in range(2):
        copy(side, side).start()

    def pair(p, carry):
        for side in range(2):
            chunk = 2 * p + side
            copy(chunk, side).wait()
            work(chunk, buffers[side])

            @pl.when(chunk + 2 < chunks)
            def _(chunk=chunk, side=side):
                copy(chunk + 2, side).start()

        return carry

    lax.fori_loop(0, chunks // 2, pair, 0)


def spans(capacity):
    marks = [0] + [m for m in (56, 80) if m < capacity] + [capacity]
    return list(zip(marks[:-1], marks[1:]))


def when_listed(listed, local, start, absent, work):
    if start == 0:
        work()
    else:
        pl.when(listed[local, start] < absent)(work)


def gather_kernel(capacity, rows_ref, out_ref, want_ref, table, digits, stage, list_a, list_b, semaphores):
    devices, held = rows_ref.shape[0], 16
    blocks = devices * held
    span = 2 * CHUNK * capacity
    digits[...] = rows_ref[:, 2 * held :, :].astype(jnp.float32).reshape(devices * 8, LANES)
    high = digits[pl.ds(0, devices, stride=8), :]
    low = digits[pl.ds(1, devices, stride=8), :]
    want_ref[...] = (2 * (high * held + low)).astype(jnp.int32)
    for half in range(2):
        rows = rows_ref[:, half * held : (half + 1) * held, :].astype(jnp.float32)
        table[pl.ds(half, blocks, stride=2), :] = rows.reshape(blocks, LANES)

    def work(chunk, listed):
        for local in range(CHUNK):
            for start, stop in spans(capacity):

                def rows(local=local, start=start, stop=stop):
                    for k in range(start, stop):
                        src = listed[local, k]
                        stage[pl.ds(2 * (local * capacity + k), 2), :] = table[pl.ds(src, 2), :]

                when_listed(listed, local, start, 2 * blocks, rows)
        out_ref[pl.ds(pl.multiple_of(chunk * span, 16), span), :] = stage[...].astype(jnp.bfloat16)

    chunk_lists(want_ref, (list_a, list_b), semaphores, work)


def row_table(blocks):
    return pltpu.VMEM((2 * (blocks + 8), LANES), jnp.float32)


def list_scratch(capacity):
    lists = pltpu.SMEM((CHUNK, LANES), jnp.int32)
    stage = pltpu.VMEM((2 * CHUNK * capacity, LANES), jnp.float32)
    return [stage, lists, lists, pltpu.SemaphoreType.DMA((2,))]


def gather_rows(rows, capacity):
    devices = rows.shape[0]
    return pl.pallas_call(
        functools.partial(gather_kernel, capacity),
        in_specs=[pl.BlockSpec(memory_space=pltpu.VMEM)],
        out_specs=[pl.BlockSpec(memory_space=pltpu.VMEM)] * 2,
        out_shape=[
            jax.ShapeDtypeStruct((devices * 2 * capacity, LANES), jnp.bfloat16),
            jax.ShapeDtypeStruct((devices, LANES), jnp.int32),
        ],
        scratch_shapes=[row_table(devices * 16), pltpu.VMEM((devices * 8, LANES), jnp.float32)]
        + list_scratch(capacity),
        compiler_params=pltpu.CompilerParams(vmem_limit_bytes=GRANT << 20),
        name=f"gather_rows_{capacity}",
    )(rows)


def product_kernel(
    capacity, slot_ref, first_ref, row_ref, count_ref, tiles_ref, in_ref, sketch_ref, out_ref,
    spread_rows, acc, sketch, sent
):
    width = 2 * capacity
    stride = width + 1
    count = count_ref[0]
    full = lax.shift_right_logical(count, GROUP_BITS)
    group = 1 << GROUP_BITS

    def spread(c, carry):
        for k in range(CHUNK):
            j = c * CHUNK + k
            source = pl.ds(pl.multiple_of(j * width, 8), width)
            spread_rows[pl.ds(j * stride, width), :] = in_ref[source, :].astype(jnp.float32)
        return carry

    def pack(c, carry):
        for k in range(CHUNK):
            j = c * CHUNK + k
            target = pl.ds(pl.multiple_of(j * width, 8), width)
            out_ref[target, :] = spread_rows[pl.ds(j * stride, width), :].astype(jnp.bfloat16)
        return carry

    def block_rows(t):
        return [pl.ds(2 * slot_ref[t] + half, LANES, stride=stride) for half in range(2)]

    def forward(first_tile, group):
        products = []
        for t in [first_tile + k for k in range(group)]:
            block = [spread_rows[rows, :].astype(jnp.bfloat16) for rows in block_rows(t)]
            block = jnp.concatenate(block, axis=1)
            products.append(jnp.dot(tiles_ref[t], block, preferred_element_type=jnp.float32))
        total = acc[...]
        for k, product in enumerate(products):
            t = first_tile + k
            row = row_ref[t]
            fresh = (t == 0) | (row_ref[jnp.maximum(t - 1, 0)] != row)
            total = jnp.where(fresh, product, total + product)
            sketch[row] = total.astype(jnp.bfloat16)
        acc[...] = total

    def backward(first_tile, group):
        parts = []
        for t in [first_tile + k for k in range(group)]:
            parts.append(
                lax.dot_general(
                    tiles_ref[t],
                    sketch[row_ref[t]],
                    (((0,), (0,)), ((), ())),
                    preferred_element_type=jnp.float32,
                )
            )
        for k, part in enumerate(parts):
            t = first_tile + k
            first = first_ref[t] == 1
            for rows, piece in zip(block_rows(t), (part[:, :LANES], part[:, LANES:])):
                spread_rows[rows, :] = piece + jnp.where(first, 0.0, spread_rows[rows, :])

    def over_tiles(work):
        def many(g, carry):
            work(g * group, group)
            return carry

        def single(t, carry):
            work(t, 1)
            return carry

        lax.fori_loop(0, full, many, 0)
        lax.fori_loop(full * group, count, single, 0)

    sketch[...] = jnp.zeros_like(sketch)
    lax.fori_loop(0, LANES // CHUNK, spread, 0)
    over_tiles(forward)
    send = pltpu.make_async_copy(sketch, sketch_ref, sent)
    send.start()
    over_tiles(backward)
    lax.fori_loop(0, LANES // CHUNK, pack, 0)
    send.wait()


def tile_products(slot_of, is_first, tile_rows, tile_count, tiles, fetched, capacity):
    sketch = (RB_DEV, LANES, 2 * LANES)
    return pl.pallas_call(
        functools.partial(product_kernel, capacity),
        in_specs=[pl.BlockSpec(memory_space=pltpu.SMEM)] * 4
        + [pl.BlockSpec(memory_space=pltpu.VMEM)] * 2,
        out_specs=[pl.BlockSpec(memory_space=pl.ANY), pl.BlockSpec(memory_space=pltpu.VMEM)],
        out_shape=[
            jax.ShapeDtypeStruct(sketch, jnp.bfloat16),
            jax.ShapeDtypeStruct(fetched.shape, jnp.bfloat16),
        ],
        scratch_shapes=[
            pltpu.VMEM((LANES * (2 * capacity + 1) + 8, LANES), jnp.float32),
            pltpu.VMEM((LANES, 2 * LANES), jnp.float32),
            pltpu.VMEM(sketch, jnp.bfloat16),
            pltpu.SemaphoreType.DMA,
        ],
        compiler_params=pltpu.CompilerParams(vmem_limit_bytes=PRODUCT_GRANT << 20),
        name=f"tile_products_{capacity}",
    )(slot_of, is_first, tile_rows, tile_count, tiles, fetched)


def sum_kernel(capacity, want_ref, in_ref, out_ref, even, odd, stage, list_a, list_b, semaphores):
    span = 2 * CHUNK * capacity
    blocks = out_ref.shape[0]
    even[...] = jnp.zeros_like(even)
    odd[...] = jnp.zeros_like(odd)
    totals = (even, odd)

    def work(chunk, listed):
        stage[...] = in_ref[pl.ds(pl.multiple_of(chunk * span, 16), span), :].astype(jnp.float32)
        for local in range(0, CHUNK, 2):

            def load(side, g, stop, local=local):
                loaded = []
                for k in range(g, min(g + SUM_GROUP, stop)):
                    w = listed[local + side, k]
                    row = stage[pl.ds(2 * ((local + side) * capacity + k), 2), :]
                    loaded.append((w, totals[side][pl.ds(w, 2), :], row))
                return loaded

            def store(side, loaded):
                for w, old, row in loaded:
                    totals[side][pl.ds(w, 2), :] = old + row

            for start, stop in spans(capacity):

                def rows(start=start, stop=stop, load=load):
                    last = load(0, start, stop)
                    turns = [(side, g) for g in range(start, stop, SUM_GROUP) for side in range(2)]
                    for here, ahead in zip(turns, turns[1:] + [None]):
                        following = load(*ahead, stop) if ahead else None
                        store(here[0], last)
                        last = following

                if start == 0:
                    rows()
                else:
                    longest = jnp.minimum(listed[local, start], listed[local + 1, start])
                    pl.when(longest < 2 * blocks)(rows)

    chunk_lists(want_ref, (list_a, list_b), semaphores, work)
    for half in range(2):
        rows = pl.ds(half, blocks, stride=2)
        out_ref[:, half * LANES : (half + 1) * LANES] = (even[rows, :] + odd[rows, :]).astype(jnp.bfloat16)


def sum_rows(want, inbound, capacity):
    blocks = want.shape[0] * 16
    return pl.pallas_call(
        functools.partial(sum_kernel, capacity),
        in_specs=[pl.BlockSpec(memory_space=pltpu.VMEM)] * 2,
        out_specs=pl.BlockSpec(memory_space=pltpu.VMEM),
        out_shape=jax.ShapeDtypeStruct((blocks, 2 * LANES), jnp.bfloat16),
        scratch_shapes=[row_table(blocks)] * 2 + list_scratch(capacity),
        compiler_params=pltpu.CompilerParams(vmem_limit_bytes=GRANT << 20),
        name=f"sum_rows_{capacity}",
    )(want, inbound)


def stripe_kernel(panel_ref, notes_ref, out_ref, rows):
    held, devices = panel_ref.shape[0], panel_ref.shape[1]
    stride = 2 * held + 1
    for s in range(held):
        for half in range(2):
            piece = panel_ref[s, :, half * LANES : (half + 1) * LANES].astype(jnp.float32)
            rows[pl.ds(half * held + s, devices, stride=stride), :] = piece

    def write(c, carry):
        for k in range(CHUNK):
            i = c * CHUNK + k
            out_ref[i, : 2 * held, :] = rows[pl.ds(i * stride, 2 * held), :].astype(jnp.bfloat16)
            out_ref[i, 2 * held :, :] = notes_ref[...]
        return carry

    lax.fori_loop(0, devices // CHUNK, write, 0)


def stripe_rows(panel, notes):
    held, devices = panel.shape[0], panel.shape[1]
    return pl.pallas_call(
        stripe_kernel,
        in_specs=[pl.BlockSpec(memory_space=pltpu.VMEM)] * 2,
        out_specs=pl.BlockSpec(memory_space=pltpu.VMEM),
        out_shape=jax.ShapeDtypeStruct((devices, 2 * held + 8, LANES), jnp.bfloat16),
        scratch_shapes=[pltpu.VMEM((devices * (2 * held + 1) + 8, LANES), jnp.float32)],
        compiler_params=pltpu.CompilerParams(vmem_limit_bytes=GRANT << 20),
        name="stripe_rows",
    )(panel, notes)


def finish_kernel(in_ref, gram_ref, left, right, blocks, sent):
    devices, held = in_ref.shape[0], in_ref.shape[1]
    stride = held + 1
    halves = (left, right)

    def spread(c, carry):
        for k in range(CHUNK):
            i = c * CHUNK + k
            for half in range(2):
                piece = in_ref[i, :, half * LANES : (half + 1) * LANES].astype(jnp.float32)
                halves[half][pl.ds(i * stride, held), :] = piece
        return carry

    lax.fori_loop(0, devices // CHUNK, spread, 0)
    sends = []
    for s in range(held):
        for half in range(2):
            piece = halves[half][pl.ds(s, devices, stride=stride), :]
            blocks[s, :, half * LANES : (half + 1) * LANES] = piece
        sends.append(pltpu.make_async_copy(blocks.at[s], gram_ref.at[s], sent.at[s]))
        sends[-1].start()
    for send in sends:
        send.wait()


def finish_gram(rows):
    devices, held, width = rows.shape
    half = pltpu.VMEM((devices * (held + 1) + 8, LANES), jnp.float32)
    return pl.pallas_call(
        finish_kernel,
        in_specs=[pl.BlockSpec(memory_space=pltpu.VMEM)],
        out_specs=pl.BlockSpec(memory_space=pl.ANY),
        out_shape=jax.ShapeDtypeStruct((held, devices, width), jnp.float32),
        scratch_shapes=[
            half,
            half,
            pltpu.VMEM((held, devices, width), jnp.float32),
            pltpu.SemaphoreType.DMA((held,)),
        ],
        compiler_params=pltpu.CompilerParams(vmem_limit_bytes=GRANT << 20),
        name="finish_gram",
    )(rows)


def exchange(x):
    return lax.all_to_all(x, AXES, split_axis=0, concat_axis=0, tiled=True)


def per_device(tiles, tile_rows, tile_cols, tile_count, block_perm, panel):
    devices = lax.axis_size(AXES)
    held = panel.shape[0]
    blocks = devices * held
    slot_ids = jnp.arange(tiles.shape[0], dtype=jnp.int32)
    is_live = slot_ids < tile_count[0]
    stored_at = block_perm[tile_cols]
    wanted, slot_of, is_first = distinct_blocks(stored_at, is_live, blocks)

    notes = jnp.stack([wanted // held, wanted % held] + [jnp.zeros_like(wanted)] * 6)
    striped = exchange(stripe_rows(panel, notes.astype(jnp.bfloat16)))
    nearest = jnp.min(striped[:, 2 * held, :].astype(jnp.float32), axis=0)
    marks = functools.reduce(jnp.logical_or, [slot_ids == c for c in CAPACITIES[:-1]])
    choice = jnp.sum((marks & (nearest < devices)).astype(jnp.int32))

    def with_capacity(capacity):
        def run():
            outgoing, want = gather_rows(striped, capacity)
            fetched = exchange(outgoing.reshape(devices, 2 * capacity, LANES))
            sketch, outbound = tile_products(
                slot_of, is_first, tile_rows, tile_count, tiles, fetched.reshape(outgoing.shape), capacity
            )
            inbound = exchange(outbound.reshape(devices, 2 * capacity, LANES))
            return sketch, sum_rows(want, inbound.reshape(outgoing.shape), capacity)

        return run

    sketch, summed = lax.switch(choice, [with_capacity(c) for c in CAPACITIES])
    gram = exchange(summed.reshape(devices, held, 2 * LANES))
    return sketch, finish_gram(gram)


def solution(mesh):
    split = P(AXES, None, None)
    line = P(AXES)
    return jax.shard_map(
        per_device,
        mesh=mesh,
        in_specs=(split, line, line, line, P(), split),
        out_specs=(split, split),
        check_vma=False,
    )
```
